128 devices in a mesh: dp: 8 (over z, core), expert: 16 (over y, x).
Axes of the slice: x: 4, y: 4, z: 4, core: 2. Of those that a mesh axis runs over, the one named last changes fastest.
Arguments:
- frames: bfloat16 [16384, 1024], P(('dp', 'expert')), may hold values from -6 to 6
- norm_gain: float32 [1024], replicated, may hold values from 0.5 to 1.5
- norm_bias: float32 [1024], replicated, may hold values from -3 to 3
- routes: int32 [16384, 2], P(('dp', 'expert')), may hold values from 0 to 31, all different within a row; in each aligned block of 128 rows (0 to 127, 128 to 255, ...) at most 16 rows name the same one
- gate_codes: int32 [16384, 2], P(('dp', 'expert')), may hold values from 1 to 255
- limits: int32 [32], replicated, may hold values from 8 to 16
- up_weight: bfloat16 [128, 1024, 1024], P(('dp', 'expert')), may hold values from -0.1875 to 0.1875
- up_bias: float32 [128, 1024], P(('dp', 'expert')), may hold values from -3 to 3
- down_weight: bfloat16 [128, 1024, 1024], P(('dp', 'expert')), may hold values from -0.09375 to 0.09375
- down_bias: float32 [32, 1024], replicated, may hold values from -2 to 2
Outputs:
- mixed: bfloat16 [16384, 1024], P(('dp', 'expert'))
- load: int32 [32], replicated
The draws below stay inside these ranges and needn't reach their ends.
Inputs may be any that keep to these rules, and one draw needn't show every extreme that they name: `routes`: in each aligned block of 128 rows (the rows of one device) no expert is named by more than 16 rows, and some block has an expert named by exactly 16 rows; the two entries of a row differ.
All inputs are finite; a program needn't handle non-finite values.
Results may differ from the reference program's by a relative error of at most 0.0051.
Values may be sent and summed in bfloat16 or wider, within the bound.
No kernel may reach another device: no remote copies, remote signals or barrier semaphores. Data moves between devices by JAX's collectives and lax.ppermute only.
A program may use at most 64 MiB of HBM per device.

```python
import math
import jax
import jax.numpy as jnp
import numpy as np
from jax import lax

D = 1024
FF = 4096
TOK_DEV = 128
EXPERTS = 32
SHARDS = 4
FF_DEV = 1024
CAP = 16
TOKENS = 16384
N_DP = 8
N_EXPERT = 16


def plant(array, rng, least, high):
    longest = array.shape.index(max(array.shape))
    spots = []
    for shift in (0, 1):
        where = [jax.random.randint(jax.random.fold_in(rng, axis), (), 0, length) for axis, length in enumerate(array.shape)]
        where[longest] = (where[longest] + shift) % array.shape[longest]
        spots.append(tuple(where))
    return array.at[spots[0]].set(least).at[spots[1]].set(high)


def level_of(own_key, shape, pieces, low, top_value):
    def one(axis_at, shards_of):
        heights = jax.random.uniform(jax.random.fold_in(jax.random.fold_in(own_key, 6), axis_at), (shards_of,), jnp.float32, low / len(pieces), top_value / len(pieces))
        return jnp.repeat(jnp.exp(heights), shape[axis_at] // shards_of).reshape((-1,) + (1,) * (len(shape) - axis_at - 1))

    gain = one(*pieces[0])
    for cut in pieces[1:]:
        gain = gain * one(*cut)
    return gain


def shared_out(key, own, number, rows, number_of, top, limit, skew):
    sequence = jax.random.permutation(key, number_of)
    packed, usual = load_shares(number_of, rows * top, limit, skew, True), load_shares(number_of, rows * top, limit, skew, False)
    places = jnp.arange(number_of)

    def named(lengths, turn):
        used = int((lengths > 0).sum())
        fixed = max(1, used // 4)
        moved = fixed + (places - fixed + turn * (used - fixed)) % max(1, number_of - fixed)
        return jnp.zeros((number_of,), jnp.int32).at[sequence[jnp.where(places < fixed, places, moved)]].set(jnp.asarray(lengths, jnp.int32))

    lengths = jnp.where(number % 4 == 0, named(packed, number // 4), named(usual, number - number // 4 - 1))
    mixed = jax.random.permutation(jax.random.fold_in(own, 3), number_of)
    giver, receiver = mixed[0:number_of // 2 * 2:2], mixed[1:number_of // 2 * 2:2]
    room = jnp.minimum(lengths[giver] - 1, limit - lengths[receiver]) // 2
    room = jnp.where((giver == sequence[0]) | (receiver == sequence[0]) | (lengths[receiver] == 0), 0, jnp.maximum(room, 0))
    moved = jax.random.randint(jax.random.fold_in(own, 4), (number_of // 2,), 0, 1 << 20) % (room + 1)
    lengths = lengths.at[giver].add(-moved).at[receiver].add(moved)
    members = jnp.searchsorted(jnp.cumsum(lengths), jnp.arange(rows * top), side="right").astype(jnp.int32)
    table = members.reshape(top, rows).T
    table = table[jax.random.permutation(jax.random.fold_in(own, 1), rows)]
    turn = jax.random.randint(jax.random.fold_in(own, 2), (rows, 1), 0, top)
    return jnp.take_along_axis(table, (jnp.arange(top)[None, :] + turn) % top, axis=1)


def load_shares(count, total, reach, lean, full):
    portions = [(1 << 20) // math.isqrt(grade ** lean) + 1 for grade in range(1, count + 1)]
    largest = reach if full else min(reach, max(-(-total // count), total * portions[0] // sum(portions)))
    least = 1 if total - largest >= count - 1 else 0
    holding, rest = [largest] + [least] * (count - 1), total - largest - least * (count - 1)
    while rest > 0:
        candidates = [i for i in range(1, count) if holding[i] < largest] or [i for i in range(1, count) if holding[i] < reach]
        whole, left = sum([portions[i] for i in candidates]), rest
        for i in candidates:
            extra = min(reach - holding[i], max(1, left * portions[i] // whole), rest)
            holding[i] = holding[i] + extra
            rest = rest - extra
    return np.array(holding)


def gaussian(stream_key, dims, scale, bound, shards=(), held_as=jnp.bfloat16):
    values = scale * jax.random.normal(stream_key, dims, jnp.float32)
    if shards:
        values = values * level_of(stream_key, dims, shards, -0.22, 0.18)
    return jnp.clip(values, -bound, bound).astype(held_as)


def setup_inputs(seed: int = 0) -> dict:
    keys = jax.random.split(jax.random.key(seed), 11)
    frames = gaussian(keys[0], (TOKENS, D), 1.0, 6.0, ((0, 128),))
    norm_gain = jnp.clip(jax.random.uniform(keys[1], (D,), jnp.float32, 0.5, 1.5), 0.5, 1.5)
    norm_bias = gaussian(keys[2], (D,), 0.5, 3.0, (), jnp.float32)
    routes_keys = jax.random.split(jax.random.fold_in(keys[3], 1), TOKENS // TOK_DEV)
    routes_turns = jax.random.permutation(jax.random.fold_in(keys[3], 3), TOKENS // TOK_DEV)
    routes = jax.vmap(lambda own, number: shared_out(jax.random.fold_in(keys[3], 2), own, number, TOK_DEV, EXPERTS, 2, CAP, 2))(routes_keys, routes_turns).reshape((TOKENS, 2))
    gate_codes = plant(jax.random.randint(keys[4], (TOKENS, 2), 1, 256), jax.random.fold_in(keys[4], 1), 1, 255).astype(jnp.int32)
    limits = plant(jax.random.randint(keys[5], (EXPERTS,), CAP // 2, CAP + 1), jax.random.fold_in(keys[5], 1), CAP // 2, CAP).astype(jnp.int32)
    up_weight = gaussian(keys[6], (EXPERTS * SHARDS, D, FF_DEV), D ** -0.5, 0.1875, ((0, 128),))
    up_bias = gaussian(keys[7], (EXPERTS * SHARDS, FF_DEV), 0.5, 3.0, ((0, 128),), jnp.float32)
    down_weight = gaussian(keys[8], (EXPERTS * SHARDS, FF_DEV, D), FF ** -0.5, 0.09375, ((0, 128),))
    down_bias = gaussian(keys[9], (EXPERTS, D), 0.3, 2.0, (), jnp.float32)
    return dict(frames=frames, norm_gain=norm_gain, norm_bias=norm_bias, routes=routes, gate_codes=gate_codes, limits=limits, up_weight=up_weight, up_bias=up_bias, down_weight=down_weight, down_bias=down_bias)


epsilon = 1e-05

def layer_norm(frames, norm_gain, norm_bias):
    values = frames.astype(jnp.float32)
    center = lax.optimization_barrier(jnp.mean(values, axis=-1, keepdims=True))
    shifted = values - center
    spread = lax.optimization_barrier(jnp.mean(shifted * shifted, axis=-1, keepdims=True))
    return (shifted * lax.rsqrt(spread + epsilon) * norm_gain + norm_bias).astype(jnp.bfloat16)

def place_slots(routes_block, limits, expert_total, capacity):
    flat_routes = routes_block.reshape(-1)
    expert_ids = jnp.arange(expert_total, dtype=jnp.int32)
    expert_hits = (flat_routes[:, None] == expert_ids[None, :]).astype(jnp.int32)
    earlier = jnp.cumsum(expert_hits, axis=0).astype(jnp.int32) - expert_hits
    slot_rank = lax.optimization_barrier(jnp.sum(earlier * expert_hits, axis=1)).astype(jnp.int32)
    slot_bound = lax.optimization_barrier(jnp.sum(expert_hits * limits[None, :], axis=1)).astype(jnp.int32)
    kept_mask = (slot_rank < slot_bound).astype(jnp.int32)
    slot_index = jnp.minimum(flat_routes * capacity + slot_rank, expert_total * capacity - 1).astype(jnp.int32)
    slot_ids = jnp.arange(expert_total * capacity, dtype=jnp.int32)
    matches = (slot_index[None, :] == slot_ids[:, None]).astype(jnp.int32) * kept_mask[None, :]
    frame_ids = jnp.arange(flat_routes.shape[0], dtype=jnp.int32) // 2
    source_frame = lax.optimization_barrier(jnp.sum(matches * frame_ids[None, :], axis=1)).astype(jnp.int32)
    filled = lax.optimization_barrier(jnp.sum(matches, axis=1)).astype(jnp.int32)
    expert_loads = lax.optimization_barrier(jnp.sum(expert_hits * kept_mask[:, None], axis=0)).astype(jnp.int32)
    return (slot_index, kept_mask, source_frame, filled, expert_loads)

def fill_slots(normed_block, source_frame, filled):
    slot_rows = jnp.take(normed_block, source_frame, axis=0)
    return slot_rows * filled[:, None].astype(jnp.bfloat16)

def combine(frames_block, returned, slot_index, kept_mask, gate_block):
    code_values = gate_block.astype(jnp.float32)
    shares = code_values / lax.optimization_barrier(jnp.sum(code_values, axis=1, keepdims=True))
    weights = shares.reshape(-1) * kept_mask.astype(jnp.float32)
    picked = jnp.take(returned, slot_index, axis=0).astype(jnp.float32)
    weighted = (picked * weights[:, None]).reshape(frames_block.shape[0], 2, frames_block.shape[1])
    return (frames_block.astype(jnp.float32) + lax.optimization_barrier(jnp.sum(weighted, axis=1))).astype(jnp.bfloat16)

def expert_rows(slot_rows, w_up, b_up, w_down, b_down):
    preact = jnp.einsum('rd,sdf->srf', slot_rows.astype(jnp.float32), w_up.astype(jnp.float32)) + b_up[:, None, :]
    hidden = jax.nn.gelu(preact, approximate=False).astype(jnp.bfloat16)
    partial_out = jnp.einsum('srf,sfd->srd', hidden.astype(jnp.float32), w_down.astype(jnp.float32))
    rounded = lax.optimization_barrier(partial_out.astype(jnp.bfloat16)).astype(jnp.float32)
    return (lax.optimization_barrier(jnp.sum(rounded, axis=0)) + b_down).astype(jnp.bfloat16)

def reference(frames, norm_gain, norm_bias, routes, gate_codes, limits, up_weight, up_bias, down_weight, down_bias):
    blocks = N_DP * N_EXPERT
    normed = layer_norm(frames, norm_gain, norm_bias).reshape(blocks, TOK_DEV, D)

    def placer(routes_block):
        return place_slots(routes_block, limits, EXPERTS, CAP)
    slot_index, kept_mask, source_frame, filled, expert_loads = jax.vmap(placer)(routes.reshape(blocks, TOK_DEV, 2))
    sent_rows = jax.vmap(fill_slots)(normed, source_frame, filled)
    by_expert = sent_rows.reshape(blocks, EXPERTS, CAP, D).transpose(1, 0, 2, 3).reshape(EXPERTS, blocks * CAP, D)
    up_grouped = up_weight.reshape(EXPERTS, SHARDS, D, FF_DEV)
    upb_grouped = up_bias.reshape(EXPERTS, SHARDS, FF_DEV)
    down_grouped = down_weight.reshape(EXPERTS, SHARDS, FF_DEV, D)

    def one_expert(operands):
        return expert_rows(operands[0], operands[1], operands[2], operands[3], operands[4])
    outputs = lax.map(one_expert, (by_expert, up_grouped, upb_grouped, down_grouped, down_bias))
    returned = outputs.reshape(EXPERTS, blocks, CAP, D).transpose(1, 0, 2, 3).reshape(blocks, EXPERTS * CAP, D)
    mixed = jax.vmap(combine)(frames.reshape(blocks, TOK_DEV, D), returned, slot_index, kept_mask, gate_codes.reshape(blocks, TOK_DEV, 2))
    return (mixed.reshape(TOKENS, D), lax.optimization_barrier(jnp.sum(expert_loads, axis=0)).astype(jnp.int32))
```

```python
import jax
import jax.numpy as jnp
from jax import lax
from jax.experimental import pallas as pl
from jax.experimental.pallas import tpu as pltpu
from jax.sharding import Mesh
from jax.sharding import PartitionSpec as P

ALL = ("z", "c", "y", "x")
ZCY = ("z", "c", "y")
EPS = 1e-05
F32 = jnp.float32
BF16 = jnp.bfloat16


def column(row):
    size = row.shape[1]
    same = lax.broadcasted_iota(jnp.int32, (size, size), 0) == lax.broadcasted_iota(
        jnp.int32, (size, size), 1
    )
    return jnp.sum(jnp.where(same, row, 0), axis=1, keepdims=True)


def slot_ranks(routes_ref, limits, frames, experts):
    ids = lax.broadcasted_iota(jnp.int32, (experts, frames), 0)
    hit = (routes_ref[0:1, :] == ids) | (routes_ref[1:2, :] == ids)
    row = lax.broadcasted_iota(jnp.int32, (frames, frames), 0)
    col = lax.broadcasted_iota(jnp.int32, (frames, frames), 1)
    earlier = (row < col).astype(BF16)
    rank = jnp.dot(hit.astype(BF16), earlier, preferred_element_type=F32).astype(jnp.int32)
    kept = hit & (rank < limits)
    return jnp.where(kept, rank, -1)


def dispatch_kernel(
    frames_hbm, gain_hbm, bias_hbm, routes_hbm, limits_hbm, low_ref, high_ref, count_ref,
    frames_ref, gain_ref, bias_ref, routes_ref, limits_ref, sems,
):
    loads = [
        pltpu.make_async_copy(source, target, sems.at[i])
        for i, (source, target) in enumerate(
            (
                (routes_hbm, routes_ref),
                (limits_hbm, limits_ref),
                (frames_hbm, frames_ref),
                (gain_hbm, gain_ref),
                (bias_hbm, bias_ref),
            )
        )
    ]
    for load in loads:
        load.start()
    for load in loads:
        load.wait()
    frames, width = frames_ref.shape
    experts = limits_ref.shape[1]
    half = low_ref.shape[0] // experts
    values = frames_ref[...].astype(F32)
    center = jnp.sum(values, axis=1, keepdims=True) * (1.0 / width)
    shifted = values - center
    spread = jnp.sum(shifted * shifted, axis=1, keepdims=True) * (1.0 / width)
    normed = (shifted * lax.rsqrt(spread + EPS) * gain_ref[...] + bias_ref[...]).astype(BF16)
    ranks = slot_ranks(routes_ref, column(limits_ref[...]), frames, experts)
    taken = (ranks >= 0).astype(F32).astype(BF16)
    ones = jnp.ones((8, frames), BF16)
    count_ref[...] = lax.dot_general(
        ones, taken, (((1,), (1,)), ((), ())), preferred_element_type=F32
    ).astype(jnp.int32)
    spots = lax.broadcasted_iota(jnp.int32, (experts, half, frames), 1)
    for part, ref in enumerate((low_ref, high_ref)):
        pick = (ranks[:, None, :] == spots + part * half).astype(F32).astype(BF16)
        rows = jnp.dot(
            pick.reshape(experts * half, frames), normed, preferred_element_type=F32
        )
        ref[...] = rows.astype(BF16)


def combine_kernel(frames_ref, low_ref, high_ref, routes_ref, gates_ref, limits_ref, out_ref):
    frames, _ = frames_ref.shape
    experts = limits_ref.shape[1]
    half = low_ref.shape[0] // experts
    ranks = slot_ranks(routes_ref, column(limits_ref[...]), frames, experts)
    codes = gates_ref[...].astype(F32)
    shares = codes / jnp.sum(codes, axis=0, keepdims=True)
    ids = lax.broadcasted_iota(jnp.int32, (experts, frames), 0)
    weights = jnp.where(routes_ref[0:1, :] == ids, shares[0:1, :], 0.0) + jnp.where(
        routes_ref[1:2, :] == ids, shares[1:2, :], 0.0
    )
    weights_hi = weights.astype(BF16)
    weights_lo = (weights - weights_hi.astype(F32)).astype(BF16)
    slots = experts * half
    owner = lax.broadcasted_iota(jnp.int32, (experts, slots), 1) // half
    spread = (owner == lax.broadcasted_iota(jnp.int32, (experts, slots), 0)).astype(BF16)
    tn = (((0,), (0,)), ((), ()))

    def wide(value):
        return lax.dot_general(value, spread, tn, preferred_element_type=F32)

    ranks_wide = wide(ranks.astype(F32).astype(BF16))
    hi_wide, lo_wide = wide(weights_hi), wide(weights_lo)
    spot = (lax.broadcasted_iota(jnp.int32, (frames, slots), 1) % half).astype(F32)
    total = frames_ref[...].astype(F32)
    for part, ref in enumerate((low_ref, high_ref)):
        here = ranks_wide == spot + float(part * half)
        for value in (hi_wide, lo_wide):
            total += jnp.dot(
                jnp.where(here, value, 0.0).astype(BF16), ref[...], preferred_element_type=F32
            )
    out_ref[...] = total.astype(BF16)


def ffn_kernel(rows_ref, up_ref, up_bias_ref, down_ref, out_ref):
    pre = jnp.dot(rows_ref[...], up_ref[...], preferred_element_type=F32) + up_bias_ref[...]
    hidden = (0.5 * pre * (1.0 + lax.erf(pre * 0.7071067811865476))).astype(BF16)
    out_ref[...] = jnp.dot(hidden, down_ref[...], preferred_element_type=F32).astype(BF16)


def merge_kernel(own_ref, other_ref, out_ref):
    out_ref[...] = (own_ref[...].astype(F32) + other_ref[...].astype(F32)).astype(BF16)


def merge(own, other):
    return call(
        merge_kernel, jax.ShapeDtypeStruct(own.shape, BF16), (own, other), own.size, 8 * 2**20
    )


def finish_kernel(own_ref, one_ref, two_ref, bias_ref, out_ref):
    total = own_ref[...].astype(F32) + one_ref[...].astype(F32) + two_ref[...].astype(F32)
    out_ref[...] = (total + bias_ref[...]).astype(BF16)


def finish(own, one, two, bias):
    return call(
        finish_kernel,
        jax.ShapeDtypeStruct(own.shape, BF16),
        (own, one, two, bias),
        own.size,
        8 * 2**20,
    )


def vmem():
    return pl.BlockSpec(memory_space=pltpu.VMEM)


def call(kernel, shapes, args, flops, limit=24 * 2**20):
    return pl.pallas_call(
        kernel,
        out_shape=shapes,
        in_specs=[vmem()] * len(args),
        out_specs=jax.tree.map(lambda _: vmem(), shapes),
        cost_estimate=pl.CostEstimate(flops=flops, bytes_accessed=4 * 2**20, transcendentals=0),
        compiler_params=pltpu.CompilerParams(vmem_limit_bytes=limit),
    )(*args)


def ring(size, step):
    return [(i, (i + step) % size) for i in range(size)]


def hop(value, axis, step):
    return lax.ppermute(value, axis, ring(lax.axis_size(axis), step))


def send(value, step):
    return hop(value, "x", step)


def per_device(frames, gain, bias, routes, gates, limits, up, up_bias, down, down_bias):
    count, width = frames.shape
    experts = down_bias.shape[0]
    capacity = 4 * count // experts
    half = capacity // 2
    routes_t, gates_t = routes.T, gates.T
    limits_c = limits[None, :]
    slots = jax.ShapeDtypeStruct((experts * half, width), BF16)
    hbm = pl.BlockSpec(memory_space=pltpu.HBM)
    low, high, counts = pl.pallas_call(
        dispatch_kernel,
        out_shape=(slots, slots, jax.ShapeDtypeStruct((8, experts), jnp.int32)),
        in_specs=[hbm] * 5,
        out_specs=(vmem(), vmem(), vmem()),
        scratch_shapes=[
            pltpu.VMEM((count, width), BF16),
            pltpu.VMEM((1, width), F32),
            pltpu.VMEM((1, width), F32),
            pltpu.VMEM((2, count), jnp.int32),
            pltpu.VMEM((1, experts), jnp.int32),
            pltpu.SemaphoreType.DMA((5,)),
        ],
    )(frames, gain[None], bias[None], routes_t, limits_c)
    load = counts + hop(counts, "c", 1)
    load = load + hop(load, "x", 1)
    load = load + hop(load, "x", 2)
    here = (lax.axis_index("z") * 2 + lax.axis_index("c")) * 4 + lax.axis_index("y")
    own_bias = lax.dynamic_slice_in_dim(down_bias, here, 1, 0)

    def ffn(rows):
        return call(
            ffn_kernel,
            jax.ShapeDtypeStruct(rows.shape, BF16),
            (rows, up[0], up_bias, down[0]),
            4 * rows.shape[0] * width * width,
            10 * 2**20,
        )

    mine1 = lax.all_to_all(low, ZCY, 0, 0, tiled=True)
    mine1, load = lax.optimization_barrier((mine1, load))
    mine2 = lax.all_to_all(high, ZCY, 0, 0, tiled=True)
    load = load + hop(load, "y", 1)
    load = load + hop(load, "y", 2)
    load = load + hop(load, "z", 1)
    load = load + hop(load, "z", 2)
    backs = []
    for k, mine in ((0, mine1), (1, mine2)):
        near, step = (1, 3) if k == 0 else (3, 1)
        ahead = send(mine, near)
        behind = send(mine, step)
        far = send(ahead, near)
        p_mine, p_ahead, p_behind, p_far = ffn(mine), ffn(ahead), ffn(behind), ffn(far)
        relay = send(p_far, near)
        p_behind = merge(p_behind, relay)
        from_near = send(p_behind, near)
        from_other = send(p_ahead, step)
        total = finish(p_mine, from_near, from_other, own_bias)
        if k == 1:
            total, load = lax.optimization_barrier((total, load))
        backs.append(lax.all_to_all(total, ZCY, 0, 0, tiled=True))
    mixed = call(
        combine_kernel,
        jax.ShapeDtypeStruct(frames.shape, BF16),
        (frames, backs[0], backs[1], routes_t, gates_t, limits_c),
        10**8,
    )
    return mixed, load[0]


def solution(mesh):
    split = Mesh(mesh.devices.reshape(4, 2, 4, 4), ALL)
    one = P(ALL, None)
    in_specs = (one, P(), P(), one, one, P(), P(ALL, None, None), one, P(ALL, None, None), P())

    return jax.shard_map(
        per_device, mesh=split, in_specs=in_specs, out_specs=(one, P()), check_vma=False
    )
```

```python
import functools

import jax
import jax.numpy as jnp
from jax import lax
from jax.experimental import pallas as pl
from jax.experimental.pallas import tpu as pltpu
from jax.sharding import Mesh
from jax.sharding import PartitionSpec as P

ALL = ("z", "c", "y", "x")
ZCY = ("z", "c", "y")
EPS = 1e-05
F32 = jnp.float32
BF16 = jnp.bfloat16
TN = (((0,), (0,)), ((), ()))
HIGH = 4
ROOM = 64
GRANT = 40 * 2**20
FFN_GRANT = None


def iota(shape, axis):
    return lax.broadcasted_iota(jnp.int32, shape, axis)


def column(row):
    size = row.shape[1]
    same = iota((size, size), 0) == iota((size, size), 1)
    return jnp.sum(jnp.where(same, row, 0.0), axis=1, keepdims=True)


def slot_ranks(first, second, limits):
    experts, frames = limits.shape[0], first.shape[1]
    ids = iota((experts, frames), 0).astype(F32)
    hit = (first == ids) | (second == ids)
    earlier = (iota((frames, frames), 0) < iota((frames, frames), 1)).astype(BF16)
    rank = jnp.dot(hit.astype(BF16), earlier, preferred_element_type=F32)
    return jnp.where(hit & (rank < limits), rank, -1.0)


def gate_weights(first, second, gate_one, gate_two, experts):
    total = gate_one + gate_two
    ids = iota((experts, first.shape[1]), 0).astype(F32)
    weights = jnp.where(first == ids, gate_one / total, 0.0) + jnp.where(
        second == ids, gate_two / total, 0.0
    )
    hi = weights.astype(BF16)
    return hi, (weights - hi.astype(F32)).astype(BF16)


def rows_of(experts, each):
    slots = experts * each
    row, start = iota((slots, experts), 0), iota((slots, experts), 1) * each
    owner = ((row >= start) & (row < start + each)).astype(F32).astype(BF16)
    before = jnp.sum((row >= start + each).astype(F32), axis=1, keepdims=True)
    return owner, iota((slots, 1), 0).astype(F32) - before * float(each)


def lanes_of(experts, each):
    slots = experts * each
    lane, start = iota((experts, slots), 1), iota((experts, slots), 0) * each
    owner = ((lane >= start) & (lane < start + each)).astype(F32).astype(BF16)
    before = jnp.sum((lane >= start + each).astype(F32), axis=0, keepdims=True)
    return owner, iota((1, slots), 1).astype(F32) - before * float(each)


def high_offsets(extra):
    experts = extra.shape[0]
    before = (iota((experts, experts), 1) < iota((experts, experts), 0)).astype(F32).astype(BF16)
    spread = jnp.broadcast_to(extra, (experts, 128)).astype(BF16)
    return jnp.dot(before, spread, preferred_element_type=F32)[:, 0:1]


def high_owners(extra, start):
    lane = iota((extra.shape[0], ROOM), 1).astype(F32)
    return ((lane >= start) & (lane < start + extra)).astype(F32).astype(BF16)


def dispatch_kernel(
    frames_hbm, gain_hbm, bias_hbm, routes_hbm, limits_hbm, payload_ref, slots_ref, count_ref,
    frames_ref, gain_ref, bias_ref, routes_ref, limits_ref, sems,
):
    loads = [
        pltpu.make_async_copy(source, target, sems.at[i])
        for i, (source, target) in enumerate(
            (
                (routes_hbm, routes_ref),
                (limits_hbm, limits_ref),
                (frames_hbm, frames_ref),
                (gain_hbm, gain_ref),
                (bias_hbm, bias_ref),
            )
        )
    ]
    for load in loads:
        load.start()
    for load in loads:
        load.wait()
    frames, width = frames_ref.shape
    experts = limits_ref.shape[1]
    values = frames_ref[...].astype(F32)
    center = jnp.sum(values, axis=1, keepdims=True) * (1.0 / width)
    shifted = values - center
    spread = jnp.sum(shifted * shifted, axis=1, keepdims=True) * (1.0 / width)
    normed = (shifted * lax.rsqrt(spread + EPS) * gain_ref[...] + bias_ref[...]).astype(BF16)
    first, second = routes_ref[0:1, :].astype(F32), routes_ref[1:2, :].astype(F32)
    ranks = slot_ranks(first, second, column(limits_ref[...].astype(F32)))
    low, half = slots_ref.shape[0] // (2 * experts), width // 2
    owner, spot = rows_of(experts, 2 * low)
    second_half = spot >= float(low)
    wide = jnp.dot(owner, ranks.astype(BF16), preferred_element_type=F32)
    pick = (wide == jnp.where(second_half, spot - float(low), spot)).astype(F32).astype(BF16)
    slots_ref[...] = jnp.where(
        second_half,
        jnp.dot(pick, normed[:, half:], preferred_element_type=F32),
        jnp.dot(pick, normed[:, :half], preferred_element_type=F32),
    ).astype(BF16)
    taken = (ranks >= 0.0).astype(F32)
    extra = jnp.maximum(jnp.sum(taken, axis=1, keepdims=True) - float(low), 0.0)
    start = high_offsets(extra)
    owners = high_owners(extra, start)
    at = iota((ROOM, 1), 0).astype(F32) - lax.dot_general(
        owners, jnp.broadcast_to(start, (experts, 128)).astype(BF16), TN, preferred_element_type=F32
    )[:, 0:1]
    wide = lax.dot_general(owners, ranks.astype(BF16), TN, preferred_element_type=F32)
    pick = (wide == at + float(low)).astype(F32).astype(BF16)
    payload_ref[0:ROOM, :] = jnp.dot(pick, normed, preferred_element_type=F32).astype(BF16)
    counts = lax.dot_general(
        jnp.ones((8, frames), BF16), taken.astype(BF16), (((1,), (1,)), ((), ())),
        preferred_element_type=F32,
    )
    lanes = (iota((experts, 128), 0) == iota((experts, 128), 1)).astype(F32).astype(BF16)
    counts = jnp.dot(counts.astype(BF16), lanes, preferred_element_type=F32)
    count_ref[...] = counts.astype(jnp.int32)
    payload_ref[ROOM : ROOM + 8, :] = jnp.zeros((8, width), BF16)
    more = jnp.maximum(counts - float(low), 0.0)
    ahead = (iota((128, 128), 0) < iota((128, 128), 1)).astype(F32).astype(BF16)
    begin = jnp.dot(more.astype(BF16), ahead, preferred_element_type=F32)
    payload_ref[ROOM : ROOM + 8, 0:128] = jnp.where(
        iota((8, 128), 0) == 0, more, begin
    ).astype(BF16)


def high_picks(experts, meta, picks_ref):
    owner, spot = rows_of(experts, 4 * HIGH)
    known = lax.dot_general(
        owner, meta[:, 0:experts], (((1,), (1,)), ((), ())), preferred_element_type=F32
    )
    lane = iota((1, 2 * ROOM), 1).astype(F32)
    for pair in range(2):
        chosen = []
        for j in (2 * pair, 2 * pair + 1):
            place = spot - float(j * HIGH)
            held, row = known[:, 8 * j : 8 * j + 1], known[:, 8 * j + 1 : 8 * j + 2] + place
            inside = (place >= 0.0) & (place < float(HIGH)) & (place < held)
            chosen.append(jnp.where(inside, row + float((j - 2 * pair) * ROOM), -1.0))
        pick = jnp.where(lane < float(ROOM), chosen[0], chosen[1]) == lane
        picks_ref[:, pair * 2 * ROOM : (pair + 1) * 2 * ROOM] = pick.astype(F32).astype(BF16)


def gather_kernel(own_hbm, left_hbm, right_hbm, far_hbm, slots_ref, meta_ref, rows, meta, picks_ref, sems):
    experts = slots_ref.shape[0] // (4 * HIGH)
    sources = (own_hbm, left_hbm, right_hbm, far_hbm)
    loads = [
        pltpu.make_async_copy(
            ref.at[pl.ds(ROOM, 8), pl.ds(0, 128)], meta.at[pl.ds(8 * j, 8), :], sems.at[j]
        )
        for j, ref in enumerate(sources)
    ]
    bulk = [
        pltpu.make_async_copy(
            ref.at[pl.ds(0, ROOM), :], rows.at[pl.ds(ROOM * j, ROOM), :], sems.at[4 + j]
        )
        for j, ref in enumerate(sources)
    ]
    for load in loads + bulk:
        load.start()
    for load in loads:
        load.wait()
    meta_ref[...] = meta[...]
    high_picks(experts, meta[...], picks_ref)
    for load in bulk:
        load.wait()
    slots_ref[...] = jnp.dot(picks_ref[...], rows[...], preferred_element_type=F32).astype(BF16)


def share_kernel(slots_ref, meta_ref, own_ref, left_ref, right_ref, far_ref, picks_ref):
    high_picks(slots_ref.shape[0] // (4 * HIGH), meta_ref[...], picks_ref)
    total = lax.dot_general(picks_ref[...], slots_ref[...], TN, preferred_element_type=F32)
    for j, ref in enumerate((own_ref, left_ref, right_ref, far_ref)):
        ref[...] = total[j * ROOM : (j + 1) * ROOM, :].astype(BF16)


def weight_kernel(
    own_ref, one_ref, two_ref, three_ref, routes_ref, gates_ref, limits_ref,
    rows_ref, hi_ref, lo_ref, high_hi_ref, high_lo_ref,
):
    experts = limits_ref.shape[1]
    frames = routes_ref.shape[1]
    half = hi_ref.shape[1] // (2 * experts)
    first, second = routes_ref[0:1, :].astype(F32), routes_ref[1:2, :].astype(F32)
    one, two = gates_ref[0:1, :].astype(F32), gates_ref[1:2, :].astype(F32)
    ranks = slot_ranks(first, second, column(limits_ref[...].astype(F32)))
    taken = (ranks >= 0.0).astype(F32)
    ranks = ranks.astype(BF16)
    hi, lo = gate_weights(first, second, one, two, experts)

    def spread(value, owner):
        return lax.dot_general(value, owner, TN, preferred_element_type=F32)

    owner, place = lanes_of(experts, 2 * half)
    second_half = place >= float(half)
    here = spread(ranks, owner) == jnp.where(second_half, place - float(half), place)
    for value, ref in ((hi, hi_ref), (lo, lo_ref)):
        chosen = jnp.where(here, spread(value, owner), 0.0)
        ref[0:frames, :] = jnp.where(second_half, 0.0, chosen).astype(BF16)
        ref[frames : 2 * frames, :] = jnp.where(second_half, chosen, 0.0).astype(BF16)
    extra = jnp.maximum(jnp.sum(taken, axis=1, keepdims=True) - float(half), 0.0)
    start = high_offsets(extra)
    owner = high_owners(extra, start)
    at = iota((1, ROOM), 1).astype(F32) - jnp.sum(owner.astype(F32) * start, axis=0, keepdims=True)
    here = spread(ranks, owner) == at + float(half)
    for value, ref in ((hi, high_hi_ref), (lo, high_lo_ref)):
        ref[...] = jnp.where(here, spread(value, owner), 0.0).astype(BF16)
    total = own_ref[...].astype(F32)
    for ref in (one_ref, two_ref, three_ref):
        total += ref[...].astype(F32)
    rows_ref[...] = total.astype(BF16)


def mix_kernel(
    frames_ref, slots_ref, hi_ref, lo_ref, rows_ref, high_hi_ref, high_lo_ref, out_ref
):
    slots, rows = slots_ref[...], rows_ref[...]
    total = jnp.dot(hi_ref[...], slots, preferred_element_type=F32)
    total += jnp.dot(lo_ref[...], slots, preferred_element_type=F32)
    base = frames_ref[...].astype(F32)
    base += jnp.dot(high_hi_ref[...], rows, preferred_element_type=F32)
    base += jnp.dot(high_lo_ref[...], rows, preferred_element_type=F32)
    frames, half = out_ref.shape[0], slots.shape[1]
    for part in range(2):
        lanes = slice(part * half, (part + 1) * half)
        out_ref[:, lanes] = (
            base[:, lanes] + total[part * frames : (part + 1) * frames, :]
        ).astype(BF16)


def ffn_kernel(sizes, adds, biases, first, *refs):
    count = len(sizes)
    blocks, others = refs[:count], refs[count : count + adds]
    up_hbm, up_bias_hbm, down_hbm, bias_hbm = refs[count + adds : count + adds + 4]
    expert = (lax.axis_index("z") * 2 + lax.axis_index("c")) * 4 + lax.axis_index("y")
    scale = jnp.where(lax.axis_index("x") == 0, 1.0, 0.0) if first else 1.0
    outs = refs[count + adds + 4 : 2 * count + adds + 4]
    rows, hidden, extra, up, down, up_bias, bias, sems = refs[2 * count + adds + 4 :]
    starts = [sum(sizes[:i]) for i in range(count)]
    loads = []

    def load(source, target):
        copy = pltpu.make_async_copy(source, target, sems.at[len(loads)])
        copy.start()
        loads.append(copy)
        return copy

    bias_copy = load(up_bias_hbm, up_bias)
    up_copy = load(up_hbm.at[0], up)
    ready = [
        load(block.at[pl.ds(0, size), :], rows.at[pl.ds(start, size), :])
        for block, size, start in zip(blocks, sizes, starts)
    ]
    late = [load(down_hbm.at[0], down)]
    if biases:
        late.append(load(bias_hbm, bias))
    for i in range(adds):
        late.append(load(others[i], extra.at[pl.ds(starts[i], sizes[i]), :]))
    bias_copy.wait()
    up_copy.wait()
    for i in range(count):
        ready[i].wait()
        part = slice(starts[i], starts[i] + sizes[i])
        pre = jnp.dot(rows[part, :], up[...], preferred_element_type=F32) + up_bias[...]
        hidden[part, :] = (0.5 * pre * (1.0 + lax.erf(pre * 0.7071067811865476))).astype(BF16)
    for copy in late:
        copy.wait()
    for i in range(count):
        part = slice(starts[i], starts[i] + sizes[i])
        total = jnp.dot(hidden[part, :], down[...], preferred_element_type=F32)
        if i in biases:
            total += bias[pl.ds(expert, 1), :] * scale
        if i < adds:
            total += extra[part, :].astype(F32)
        outs[i][...] = total.astype(BF16)


def vmem():
    return pl.BlockSpec(memory_space=pltpu.VMEM)


def call(kernel, shapes, args, flops, limit=10 * 2**20, scratch=()):
    return pl.pallas_call(
        kernel,
        out_shape=shapes,
        in_specs=[vmem()] * len(args),
        out_specs=jax.tree.map(lambda _: vmem(), shapes),
        scratch_shapes=scratch,
        cost_estimate=pl.CostEstimate(
            flops=flops, bytes_accessed=4 * 2**20, transcendentals=0
        ),
        compiler_params=pltpu.CompilerParams(vmem_limit_bytes=limit),
    )(*args)


def merge_kernel(own_ref, other_ref, own_two_ref, other_two_ref, out_ref, out_two_ref):
    out_ref[...] = (own_ref[...].astype(F32) + other_ref[...].astype(F32)).astype(BF16)
    out_two_ref[...] = (own_two_ref[...].astype(F32) + other_two_ref[...].astype(F32)).astype(BF16)


def packing(sources, low, part):
    row = iota((sources * low, sources), 0)
    source = jnp.sum(
        (row >= (iota((sources * low, sources), 1) + 1) * low).astype(F32), axis=1, keepdims=True
    )
    at = iota((sources * low, 1), 0).astype(F32) + (source + float(part)) * float(low)
    lane = iota((sources * low, 2 * sources * low), 1).astype(F32)
    return (lane == at).astype(F32).astype(BF16)


def pack_kernel(low, slots_ref, count_ref, top_ref, bot_ref):
    size, half = slots_ref.shape
    size //= 2
    rows = size // 2
    for part in range(2):
        pick = packing(rows // low, low, part)
        lanes = slice(part * half, (part + 1) * half)
        for i, ref in enumerate((top_ref, bot_ref)):
            block = slots_ref[i * size : (i + 1) * size, :]
            ref[0:rows, lanes] = jnp.dot(pick, block, preferred_element_type=F32).astype(BF16)
    top_ref[rows : rows + 8, :] = jnp.zeros((8, 2 * half), BF16)
    top_ref[rows : rows + 8, 0:128] = count_ref[...].astype(F32).astype(BF16)


def finish_kernel(low, *refs):
    out_ref = refs[-1]
    size, half = out_ref.shape[0] // 2, out_ref.shape[1]
    sources = size // (2 * low)
    row = iota((size, sources), 0)
    source = jnp.sum(
        (row >= (iota((size, sources), 1) + 1) * (2 * low)).astype(F32), axis=1, keepdims=True
    )
    place = iota((size, 1), 0).astype(F32) - source * float(2 * low)
    second_half = place >= float(low)
    at = source * float(low) + jnp.where(second_half, place - float(low), place)
    spread = (iota((size, size // 2), 1).astype(F32) == at).astype(F32).astype(BF16)
    for part in range(2):
        own, other = (ref[...].astype(F32) for ref in refs[2 * part : 2 * part + 2])
        total = (own + other).astype(BF16)
        out_ref[part * size : (part + 1) * size, :] = jnp.where(
            second_half,
            jnp.dot(spread, total[:, half:], preferred_element_type=F32),
            jnp.dot(spread, total[:, :half], preferred_element_type=F32),
        ).astype(BF16)


def hop(value, axis, step):
    size = lax.axis_size(axis)
    return lax.ppermute(value, axis, [(i, (i + step) % size) for i in range(size)])


def send(value, step):
    return hop(value, "x", step)


def exchange(value):
    return lax.all_to_all(value, ZCY, 0, 0, tiled=True)


def per_device(frames, gain, bias, routes, gates, limits, up, up_bias, down, down_bias):
    count, width = frames.shape
    experts = down_bias.shape[0]
    capacity = 4 * count // experts
    low = capacity - HIGH
    limits_r = limits[None, :]
    hbm = pl.BlockSpec(memory_space=pltpu.HBM)
    shape = jax.ShapeDtypeStruct
    payload, slots, counts = pl.pallas_call(
        dispatch_kernel,
        out_shape=(
            shape((ROOM + 8, width), BF16),
            shape((2 * experts * low, width // 2), BF16),
            shape((8, 128), jnp.int32),
        ),
        in_specs=[hbm] * 5,
        out_specs=(vmem(), vmem(), vmem()),
        scratch_shapes=[
            pltpu.VMEM((count, width), BF16),
            pltpu.VMEM((1, width), F32),
            pltpu.VMEM((1, width), F32),
            pltpu.VMEM((2, count), jnp.int32),
            pltpu.VMEM((1, experts), jnp.int32),
            pltpu.SemaphoreType.DMA((5,)),
        ],
    )(frames, gain[None], bias[None], routes.T, limits_r)

    def ffn(blocks, sizes, others=(), biases=(), first=False):
        n, adds, total = len(blocks), len(others), sum(sizes)
        return pl.pallas_call(
            functools.partial(ffn_kernel, sizes, adds, biases, first),
            out_shape=tuple(shape((size, width), BF16) for size in sizes),
            in_specs=[hbm] * (n + adds + 4),
            out_specs=(vmem(),) * n,
            scratch_shapes=[
                pltpu.VMEM((total, width), BF16),
                pltpu.VMEM((total, width), BF16),
                pltpu.VMEM((max(sum(sizes[:adds]), 16), width), BF16),
                pltpu.VMEM((width, width), BF16),
                pltpu.VMEM((width, width), BF16),
                pltpu.VMEM((1, width), F32),
                pltpu.VMEM((experts, width), F32),
                pltpu.SemaphoreType.DMA((n + adds + 4,)),
            ],
            compiler_params=pltpu.CompilerParams(vmem_limit_bytes=FFN_GRANT),
            cost_estimate=pl.CostEstimate(
                flops=4 * total * width * width, bytes_accessed=4 * 2**20, transcendentals=0
            ),
        )(*blocks, *others, up, up_bias, down, down_bias)

    from_left = send(payload, 1)
    from_right = send(payload, 3)
    from_far = send(payload, 2)
    mine = exchange(slots)
    high_slots, meta = pl.pallas_call(
        gather_kernel,
        out_shape=(
            shape((experts * 4 * HIGH, width), BF16),
            shape((32, 128), BF16),
        ),
        in_specs=[hbm] * 4,
        out_specs=(vmem(), vmem()),
        scratch_shapes=[
            pltpu.VMEM((4 * ROOM, width), BF16),
            pltpu.VMEM((32, 128), BF16),
            pltpu.VMEM((experts * 4 * HIGH, 4 * ROOM), BF16),
            pltpu.SemaphoreType.DMA((8,)),
        ],
        compiler_params=pltpu.CompilerParams(vmem_limit_bytes=GRANT),
        cost_estimate=pl.CostEstimate(
            flops=10**9, bytes_accessed=4 * 2**20, transcendentals=0
        ),
    )(payload, from_left, from_right, from_far)
    high = exchange(high_slots)

    size = experts * low // 2
    counts = counts + hop(counts, "c", 1)
    counts = counts + hop(counts, "y", 1)
    halves = call(
        functools.partial(pack_kernel, low),
        (shape((size + 8, width), BF16), shape((size, width), BF16)),
        (mine, counts),
        10**9,
    )
    top, bot = halves
    ahead = [send(top, 1), send(bot, 3)]
    behind = [send(top, 3), send(bot, 1)]
    far = [send(ahead[0], 1), send(ahead[1], 3)]
    p_ahead = ffn(ahead, (size,) * 2)
    other = [send(p_ahead[0], 3), send(p_ahead[1], 1)]
    p_behind = ffn(behind, (size,) * 2)
    tall = experts * 4 * HIGH
    *p_far, p_high = ffn((*far, high), (size, size, tall), (), (2,), True)
    relay = [send(p_far[0], 1), send(p_far[1], 3)]
    p_own = ffn(halves, (size, size), other, (0, 1))
    part = shape((size, width), BF16)
    joined = call(
        merge_kernel, (part, part), (p_behind[0], relay[0], p_behind[1], relay[1]), 2 * size * width
    )
    both = [send(joined[0], 1), send(joined[1], 3)]
    load = sum(
        piece[size : size + 8, 0:128].astype(F32) for piece in (top, ahead[0], behind[0], far[0])
    ).astype(jnp.int32)
    load = load + hop(load, "y", 2)
    load = load + hop(load, "z", 1)
    load = load + hop(load, "z", 2)
    back_high = exchange(p_high)
    total = call(
        functools.partial(finish_kernel, low),
        shape((2 * experts * low, width // 2), BF16),
        (p_own[0], both[0], p_own[1], both[1]),
        10**9,
    )
    back = exchange(total)
    frame_part = shape((count, width), BF16)
    weights = shape((2 * count, 2 * experts * low), BF16)
    high_part = shape((ROOM, width), BF16)
    s_own, s_left, s_right, s_far = call(
        share_kernel,
        (high_part,) * 4,
        (back_high, meta),
        10**9,
        scratch=(pltpu.VMEM((experts * 4 * HIGH, 4 * ROOM), BF16),),
    )
    three = send(s_far, 2)
    one = send(s_right, 1)
    two = send(s_left, 3)
    gate_part = shape((count, ROOM), BF16)
    rows_high, hi, lo, high_hi, high_lo = call(
        weight_kernel,
        (high_part, weights, weights, gate_part, gate_part),
        (s_own, one, two, three, routes.T, gates.T, limits_r),
        10**9,
    )
    mixed = call(mix_kernel, frame_part, (frames, back, hi, lo, rows_high, high_hi, high_lo), 10**9)
    return mixed, load[0, :experts]


def solution(mesh):
    split = Mesh(mesh.devices.reshape(4, 2, 4, 4), ALL)
    each = P(ALL, None)
    in_specs = (each, P(), P(), each, each, P(), P(ALL, None, None), each, P(ALL, None, None), P())

    return jax.shard_map(
        per_device, mesh=split, in_specs=in_specs, out_specs=(each, P()), check_vma=False
    )
```

```python
import functools

import jax
import jax.numpy as jnp
from jax import lax
from jax.experimental import pallas as pl
from jax.experimental.pallas import tpu as pltpu
from jax.sharding import Mesh
from jax.sharding import PartitionSpec as P

ALL = ("z", "c", "y", "x")
ZCY = ("z", "c", "y")
EPS = 1e-05
F32 = jnp.float32
BF16 = jnp.bfloat16
TN = (((0,), (0,)), ((), ()))
HIGH = 4


def iota(shape, axis):
    return lax.broadcasted_iota(jnp.int32, shape, axis)


def column(row):
    size = row.shape[1]
    same = iota((size, size), 0) == iota((size, size), 1)
    return jnp.sum(jnp.where(same, row, 0.0), axis=1, keepdims=True)


def slot_ranks(first, second, limits):
    experts, frames = limits.shape[0], first.shape[1]
    ids = iota((experts, frames), 0).astype(F32)
    hit = (first == ids) | (second == ids)
    earlier = (iota((frames, frames), 0) < iota((frames, frames), 1)).astype(BF16)
    rank = jnp.dot(hit.astype(BF16), earlier, preferred_element_type=F32)
    return jnp.where(hit & (rank < limits), rank, -1.0)


def gate_weights(first, second, gate_one, gate_two, experts):
    total = gate_one + gate_two
    ids = iota((experts, first.shape[1]), 0).astype(F32)
    weights = jnp.where(first == ids, gate_one / total, 0.0) + jnp.where(
        second == ids, gate_two / total, 0.0
    )
    hi = weights.astype(BF16)
    return hi, (weights - hi.astype(F32)).astype(BF16)


def rows_of(experts, each):
    slots = experts * each
    row, start = iota((slots, experts), 0), iota((slots, experts), 1) * each
    owner = ((row >= start) & (row < start + each)).astype(F32).astype(BF16)
    before = jnp.sum((row >= start + each).astype(F32), axis=1, keepdims=True)
    return owner, iota((slots, 1), 0).astype(F32) - before * float(each)


def lanes_of(experts, each):
    slots = experts * each
    lane, start = iota((experts, slots), 1), iota((experts, slots), 0) * each
    owner = ((lane >= start) & (lane < start + each)).astype(F32).astype(BF16)
    before = jnp.sum((lane >= start + each).astype(F32), axis=0, keepdims=True)
    return owner, iota((1, slots), 1).astype(F32) - before * float(each)


def dispatch_kernel(
    frames_hbm, gain_hbm, bias_hbm, routes_hbm, gates_hbm, limits_hbm, payload_ref, slots_ref,
    frames_ref, gain_ref, bias_ref, routes_ref, gates_ref, limits_ref, sems,
):
    loads = [
        pltpu.make_async_copy(source, target, sems.at[i])
        for i, (source, target) in enumerate(
            (
                (routes_hbm, routes_ref),
                (limits_hbm, limits_ref),
                (gates_hbm, gates_ref),
                (frames_hbm, frames_ref),
                (gain_hbm, gain_ref),
                (bias_hbm, bias_ref),
            )
        )
    ]
    for load in loads:
        load.start()
    for load in loads:
        load.wait()
    frames, width = frames_ref.shape
    experts = limits_ref.shape[1]
    values = frames_ref[...].astype(F32)
    center = jnp.sum(values, axis=1, keepdims=True) * (1.0 / width)
    shifted = values - center
    spread = jnp.sum(shifted * shifted, axis=1, keepdims=True) * (1.0 / width)
    normed = (shifted * lax.rsqrt(spread + EPS) * gain_ref[...] + bias_ref[...]).astype(BF16)
    payload_ref[0:frames, :] = normed
    first, second = routes_ref[0:1, :].astype(F32), routes_ref[1:2, :].astype(F32)
    one, two = gates_ref[0:1, :].astype(F32), gates_ref[1:2, :].astype(F32)
    place = iota((8, frames), 0)
    meta = jnp.where(
        place == 0, first, jnp.where(place == 1, second, jnp.where(place == 2, one, two))
    )
    payload_ref[frames : frames + 8, :] = jnp.zeros((8, width), BF16)
    payload_ref[frames : frames + 8, 0:frames] = meta.astype(BF16)
    ranks = slot_ranks(first, second, column(limits_ref[...].astype(F32)))
    capacity = slots_ref.shape[0] // experts
    low = float(capacity - HIGH)
    owner, spot = rows_of(experts, capacity)
    wide = jnp.dot(owner, ranks.astype(BF16), preferred_element_type=F32)
    pick = ((wide == spot) & (spot < low)).astype(F32).astype(BF16)
    slots_ref[...] = jnp.dot(pick, normed, preferred_element_type=F32).astype(BF16)
    taken = (ranks >= 0.0).astype(F32).astype(BF16)
    counts = lax.dot_general(
        jnp.ones((8, frames), BF16), taken, (((1,), (1,)), ((), ())), preferred_element_type=F32
    )
    lanes = (iota((experts, 128), 0) == iota((experts, 128), 1)).astype(F32).astype(BF16)
    counts = jnp.dot(counts.astype(BF16), lanes, preferred_element_type=F32)[0:1, :]
    slots_ref[:, 0:128] = jnp.where(
        spot == low, counts, slots_ref[:, 0:128].astype(F32)
    ).astype(BF16)


def gather_kernel(own_ref, left_ref, right_ref, far_ref, limits_ref, slots_ref, meta_ref):
    experts = limits_ref.shape[1]
    frames = own_ref.shape[0] - 8
    base = float(4 * frames // experts - HIGH)
    limits = column(limits_ref[...].astype(F32))
    owner, spot = rows_of(experts, 4 * HIGH)
    total = jnp.zeros((experts * 4 * HIGH, own_ref.shape[1]), F32)
    for j, ref in enumerate((own_ref, left_ref, right_ref, far_ref)):
        meta = ref[frames : frames + 8, 0:frames]
        meta_ref[8 * j : 8 * j + 8, :] = meta
        known = meta.astype(F32)
        ranks = slot_ranks(known[0:1, :], known[1:2, :], limits)
        wide = jnp.dot(owner, ranks.astype(BF16), preferred_element_type=F32)
        inside = (spot >= float(j * HIGH)) & (spot < float((j + 1) * HIGH))
        pick = ((wide == spot - float(j * HIGH) + base) & inside).astype(F32).astype(BF16)
        total += jnp.dot(pick, ref[0:frames, :], preferred_element_type=F32)
    slots_ref[...] = total.astype(BF16)


def share_kernel(
    slots_ref, meta_ref, limits_ref, frames_ref, base_ref, left_ref, right_ref, far_ref, hi_ref, lo_ref,
    mix_ref,
):
    experts = limits_ref.shape[1]
    frames = frames_ref.shape[0]
    capacity = 4 * frames // experts
    limits = column(limits_ref[...].astype(F32))
    owner, spot = lanes_of(experts, 4 * HIGH)

    def spread(value, owner):
        return lax.dot_general(value, owner, TN, preferred_element_type=F32)

    for j in range(4):
        known = meta_ref[8 * j : 8 * j + 8, :].astype(F32)
        first, second = known[0:1, :], known[1:2, :]
        ranks = slot_ranks(first, second, limits).astype(BF16)
        hi, lo = gate_weights(first, second, known[2:3, :], known[3:4, :], experts)
        inside = (spot >= float(j * HIGH)) & (spot < float((j + 1) * HIGH))
        here = inside & (
            spread(ranks, owner) == spot - float(j * HIGH) + float(capacity - HIGH)
        )
        for k, value in enumerate((hi, lo)):
            mix_ref[(4 * k + j) * frames : (4 * k + j + 1) * frames, :] = jnp.where(
                here, spread(value, owner), 0.0
            ).astype(BF16)
        if j == 0:
            own, place = lanes_of(experts, capacity)
            low = (spread(ranks, own) == place) & (place < float(capacity - HIGH))
            hi_ref[...] = jnp.where(low, spread(hi, own), 0.0).astype(BF16)
            lo_ref[...] = jnp.where(low, spread(lo, own), 0.0).astype(BF16)
    half = 4 * frames
    slots = slots_ref[...]
    total = jnp.dot(mix_ref[0:half, :], slots, preferred_element_type=F32)
    total += jnp.dot(mix_ref[half : 2 * half, :], slots, preferred_element_type=F32)
    base_ref[...] = total[0:frames, :] + frames_ref[...].astype(F32)
    for j, ref in ((1, left_ref), (2, right_ref), (3, far_ref)):
        ref[...] = total[j * frames : (j + 1) * frames, :].astype(BF16)


def mix_kernel(base_ref, one_ref, two_ref, three_ref, slots_ref, hi_ref, lo_ref, out_ref):
    total = base_ref[...] + one_ref[...].astype(F32) + two_ref[...].astype(F32)
    total += three_ref[...].astype(F32)
    for ref in (hi_ref, lo_ref):
        total += jnp.dot(ref[...], slots_ref[...], preferred_element_type=F32)
    out_ref[...] = total.astype(BF16)


def ffn_kernel(count, adds, *refs):
    blocks, others = refs[:count], refs[count : count + adds]
    up_ref, up_bias_ref, down_ref, bias_ref = refs[count + adds : count + adds + 4]
    outs = refs[count + adds + 4 :]
    for i, (block, out) in enumerate(zip(blocks, outs)):
        rows = block[0 : out.shape[0], :]
        pre = jnp.dot(rows, up_ref[...], preferred_element_type=F32) + up_bias_ref[...]
        hidden = (0.5 * pre * (1.0 + lax.erf(pre * 0.7071067811865476))).astype(BF16)
        total = jnp.dot(hidden, down_ref[...], preferred_element_type=F32) + bias_ref[...]
        if adds:
            total += others[i][...].astype(F32)
        out[...] = total.astype(BF16)


def vmem():
    return pl.BlockSpec(memory_space=pltpu.VMEM)


def call(kernel, shapes, args, flops, limit=10 * 2**20, scratch=()):
    return pl.pallas_call(
        kernel,
        out_shape=shapes,
        in_specs=[vmem()] * len(args),
        out_specs=jax.tree.map(lambda _: vmem(), shapes),
        scratch_shapes=scratch,
        cost_estimate=pl.CostEstimate(
            flops=flops, bytes_accessed=4 * 2**20, transcendentals=0
        ),
        compiler_params=pltpu.CompilerParams(vmem_limit_bytes=limit),
    )(*args)


def merge_kernel(own_ref, other_ref, own_two_ref, other_two_ref, out_ref, out_two_ref):
    out_ref[...] = (own_ref[...].astype(F32) + other_ref[...].astype(F32)).astype(BF16)
    out_two_ref[...] = (own_two_ref[...].astype(F32) + other_two_ref[...].astype(F32)).astype(BF16)


def packing(sources, capacity):
    low = capacity - HIGH
    shape = (sources * low, sources * capacity)
    row = iota((sources * low, sources), 0)
    source = jnp.sum(
        (row >= (iota((sources * low, sources), 1) + 1) * low).astype(F32), axis=1, keepdims=True
    )
    at = iota((sources * low, 1), 0).astype(F32) + source * float(HIGH)
    return (iota(shape, 1).astype(F32) == at).astype(F32).astype(BF16)


def pack_kernel(capacity, slots_ref, top_ref, bot_ref):
    size = slots_ref.shape[0] // 2
    sources = size // capacity
    pick = packing(sources, capacity)
    rows = pick.shape[0]
    spare = (iota((8, sources), 1) * capacity + capacity - HIGH, iota((8, size), 1))
    mark = jnp.zeros((8, size), F32)
    for i in range(sources):
        mark += (spare[1] == i * capacity + capacity - HIGH).astype(F32)
    for part, ref in enumerate((top_ref, bot_ref)):
        block = slots_ref[part * size : (part + 1) * size, :]
        ref[0:rows, :] = jnp.dot(pick, block, preferred_element_type=F32).astype(BF16)
        ref[rows : rows + 8, :] = jnp.zeros((8, ref.shape[1]), BF16)
        ref[rows : rows + 8, 0:128] = jnp.dot(
            mark.astype(BF16), block[:, 0:128], preferred_element_type=F32
        ).astype(BF16)


def unpacking(sources, capacity):
    low = capacity - HIGH
    row = iota((sources * capacity, sources), 0)
    source = jnp.sum(
        (row >= (iota((sources * capacity, sources), 1) + 1) * capacity).astype(F32),
        axis=1,
        keepdims=True,
    )
    place = iota((sources * capacity, 1), 0).astype(F32) - source * float(capacity)
    at = jnp.where(place < float(low), source * float(low) + place, -1.0)
    lane = iota((sources * capacity, sources * low), 1).astype(F32)
    return (lane == at).astype(F32).astype(BF16)


def finish_kernel(capacity, *refs):
    out_ref = refs[-1]
    size = out_ref.shape[0] // 2
    spread = unpacking(size // capacity, capacity)
    for part in range(2):
        own, other = (ref[...].astype(F32) for ref in refs[2 * part : 2 * part + 2])
        total = (own + other).astype(BF16)
        out_ref[part * size : (part + 1) * size, :] = jnp.dot(
            spread, total, preferred_element_type=F32
        ).astype(BF16)


def hop(value, axis, step):
    size = lax.axis_size(axis)
    return lax.ppermute(value, axis, [(i, (i + step) % size) for i in range(size)])


def send(value, step):
    return hop(value, "x", step)


def exchange(value):
    return lax.all_to_all(value, ZCY, 0, 0, tiled=True)


def per_device(frames, gain, bias, routes, gates, limits, up, up_bias, down, down_bias):
    count, width = frames.shape
    experts = down_bias.shape[0]
    capacity = 4 * count // experts
    low = capacity - HIGH
    limits_r = limits[None, :]
    hbm = pl.BlockSpec(memory_space=pltpu.HBM)
    shape = jax.ShapeDtypeStruct
    payload, slots = pl.pallas_call(
        dispatch_kernel,
        out_shape=(shape((count + 8, width), BF16), shape((experts * capacity, width), BF16)),
        in_specs=[hbm] * 6,
        out_specs=(vmem(), vmem()),
        scratch_shapes=[
            pltpu.VMEM((count, width), BF16),
            pltpu.VMEM((1, width), F32),
            pltpu.VMEM((1, width), F32),
            pltpu.VMEM((2, count), jnp.int32),
            pltpu.VMEM((2, count), jnp.int32),
            pltpu.VMEM((1, experts), jnp.int32),
            pltpu.SemaphoreType.DMA((6,)),
        ],
    )(frames, gain[None], bias[None], routes.T, gates.T, limits_r)
    here = (lax.axis_index("z") * 2 + lax.axis_index("c")) * 4 + lax.axis_index("y")
    own_bias = lax.dynamic_slice_in_dim(down_bias, here, 1, 0)
    first_bias = jnp.where(lax.axis_index("x") == 0, own_bias, 0.0)
    no_bias = jnp.zeros_like(own_bias)

    def ffn(blocks, size, extra=no_bias, others=()):
        n = len(blocks)
        return call(
            functools.partial(ffn_kernel, n, len(others)),
            (shape((size, width), BF16),) * n,
            (*blocks, *others, up[0], up_bias, down[0], extra),
            4 * n * size * width * width,
        )

    from_left = send(payload, 1)
    from_right = send(payload, 3)
    from_far = send(payload, 2)
    mine = exchange(slots)
    high_slots, meta = call(
        gather_kernel,
        (shape((experts * 4 * HIGH, width), BF16), shape((32, count), BF16)),
        (payload, from_left, from_right, from_far, limits_r),
        10**9,
    )
    high = exchange(high_slots)

    size = experts * low // 2
    packed = shape((size + 8, width), BF16)
    halves = call(functools.partial(pack_kernel, capacity), (packed, packed), (mine,), 10**9)
    load = jnp.zeros((experts,), F32)
    top, bot = halves
    ahead = [send(top, 1), send(bot, 3)]
    behind = [send(top, 3), send(bot, 1)]
    far = [send(ahead[0], 1), send(ahead[1], 3)]
    p_ahead = ffn(ahead, size)
    other = [send(p_ahead[0], 3), send(p_ahead[1], 1)]
    p_far = ffn(far, size)
    relay = [send(p_far[0], 1), send(p_far[1], 3)]
    p_behind = ffn(behind, size)
    p_own = ffn(halves, size, own_bias, other)
    part = shape((size, width), BF16)
    joined = call(
        merge_kernel, (part, part), (p_behind[0], relay[0], p_behind[1], relay[1]), 2 * size * width
    )
    both = [send(joined[0], 1), send(joined[1], 3)]
    for piece in (*halves, *ahead, *behind, *far):
        load = load + piece[size, :experts].astype(F32)
    (p_high,) = ffn([high], experts * 4 * HIGH, first_bias)
    back_high = exchange(p_high)
    total = call(
        functools.partial(finish_kernel, capacity),
        shape((experts * capacity, width), BF16),
        (p_own[0], both[0], p_own[1], both[1]),
        10**9,
    )
    back = exchange(total)
    frame_part = shape((count, width), BF16)
    weights = shape((count, experts * capacity), BF16)
    base, s_left, s_right, s_far, hi, lo = call(
        share_kernel,
        (shape((count, width), F32), frame_part, frame_part, frame_part, weights, weights),
        (back_high, meta, limits_r, frames),
        10**9,
        20 * 2**20,
        (pltpu.VMEM((8 * count, experts * 4 * HIGH), BF16),),
    )
    one = send(s_right, 1)
    two = send(s_left, 3)
    three = send(s_far, 2)
    mixed = call(mix_kernel, frame_part, (base, one, two, three, back, hi, lo), 10**9)
    return mixed, load.astype(jnp.int32)


def solution(mesh):
    split = Mesh(mesh.devices.reshape(4, 2, 4, 4), ALL)
    each = P(ALL, None)
    in_specs = (each, P(), P(), each, each, P(), P(ALL, None, None), each, P(ALL, None, None), P())

    return jax.shard_map(
        per_device, mesh=split, in_specs=in_specs, out_specs=(each, P()), check_vma=False
    )
```
